256 devices in a mesh: chain: 128 (over y, z, x), grp: 2 (over core).
Axes of the slice: x: 4, y: 4, z: 8, core: 2. Of those that a mesh axis runs over, the one named last changes fastest.
Arguments:
- codes: bfloat16 [2, 16384, 6144], P(None, ('chain', 'grp')), may hold values from -6 to 6
- exponents: int32 [2, 512, 6144], P(None, ('chain', 'grp')), may hold values from -2 to 2
- column_map: int32 [256], replicated, may hold values from 0 to 255, each once
- row_order: int32 [256], replicated, may hold values from 0 to 255, each once
Outputs:
- rollout: bfloat16 [2, 6144, 16384], P(None, ('chain', 'grp'))
- block_sums: float32 [2, 6144, 512], P(None, ('chain', 'grp'))
The draws below stay inside these ranges and needn't reach their ends.
All inputs are finite; a program needn't handle non-finite values.
Results may differ from the reference program's by a relative error of at most 0.001.
Values may be sent and summed in bfloat16 or wider, within the bound.
A program may use at most 64 MiB of HBM per device.

```python
import jax
import jax.numpy as jnp

R = 16384
C = 6144
LAYERS = 2
N_CHAIN = 128
N_GRP = 2


def plant(result, key, low, largest):
    shape = result.shape
    place = [jax.random.randint(jax.random.fold_in(key, axis), (), 0, shape[axis]) for axis in range(len(shape))]
    result = result.at[tuple(place)].set(low)
    longest = shape.index(max(shape))
    place[longest] = (place[longest] + 1) % shape[longest]
    return result.at[tuple(place)].set(largest)


def block_levels(stream_key, extent, pieces, least, largest):
    def one(dim, parts):
        heights = jax.random.uniform(jax.random.fold_in(jax.random.fold_in(stream_key, 6), dim), (parts,), jnp.float32, least / len(pieces), largest / len(pieces))
        return jnp.repeat(jnp.exp(heights), extent[dim] // parts).reshape((-1,) + (1,) * (len(extent) - dim - 1))

    factor_of = one(*pieces[0])
    for cut in pieces[1:]:
        factor_of = factor_of * one(*cut)
    return factor_of


def gaussian(rng, shape, deviation, limit, shards=(), kind=jnp.bfloat16):
    result = jax.random.normal(rng, shape, jnp.float32) * deviation
    if len(shards) > 0:
        result = block_levels(rng, shape, shards, -0.22, 0.18) * result
    return jnp.clip(result, min=-limit, max=limit).astype(kind)


def setup_inputs(seed: int = 0) -> dict:
    arg_keys = jax.random.split(jax.random.key(seed), 5)
    return {
        "codes": gaussian(arg_keys[0], (LAYERS, R, C), 1.0, 6.0, ((1, 256),)),
        "exponents": plant(jax.random.randint(arg_keys[1], (LAYERS, R // 32, C), -2, 3), jax.random.fold_in(arg_keys[1], 1), -2, 2).astype(jnp.int32),
        "column_map": jax.random.permutation(arg_keys[2], N_CHAIN * N_GRP).astype(jnp.int32),
        "row_order": jax.random.permutation(arg_keys[3], N_CHAIN * N_GRP).astype(jnp.int32),
    }


def reference(codes, exponents, column_map, row_order):
    devices = N_CHAIN * N_GRP
    col_width = C // devices
    row_count = R // devices
    scaling = jnp.exp2(exponents.astype(jnp.float32))
    values = (codes.astype(jnp.float32) * jnp.repeat(scaling, 32, axis=1)).astype(jnp.bfloat16)
    col_index = (column_map[:, None] * col_width + jnp.arange(col_width, dtype=jnp.int32)[None, :]).reshape(-1)
    row_index = (row_order[:, None] * row_count + jnp.arange(row_count, dtype=jnp.int32)[None, :]).reshape(-1)
    picked = jnp.take(values, row_index.astype(jnp.int32), axis=1)
    picked = jnp.take(picked, col_index.astype(jnp.int32), axis=2)
    rollout = jnp.transpose(picked, (0, 2, 1))
    block_sums = rollout.astype(jnp.float32).reshape(LAYERS, C, R // 32, 32).sum(axis=-1)
    return rollout, block_sums
```

```python
import functools

import jax
import jax.numpy as jnp
from jax import lax
from jax.experimental import pallas as pl
from jax.experimental.pallas import tpu as pltpu
from jax.sharding import PartitionSpec as P

MESH = pl.DeviceIdType.MESH
BLOCK = 32
LANES = 128


def exchange(sizes, codes_hbm, exps_hbm, cmap_hbm, recv, codes, exps, cmap, turned, send, load_sem, own_sem, send_sem, recv_sem):
    x_size, y_size, z_size, g_size = sizes
    devices = x_size * y_size * z_size * g_size
    layers, rows, width = codes.shape
    col_width = width // devices
    chain, g = lax.axis_index("chain"), lax.axis_index("grp")
    x, z, y = chain % x_size, (chain // x_size) % z_size, chain // (x_size * z_size)
    me = chain * g_size + g

    loads = [
        pltpu.make_async_copy(codes_hbm, codes, load_sem.at[0]),
        pltpu.make_async_copy(exps_hbm, exps, load_sem.at[1]),
        pltpu.make_async_copy(cmap_hbm, cmap, load_sem.at[2]),
    ]
    for load in loads:
        load.start()

    def peer(step):
        dz, dx = step % z_size, (step // z_size) % x_size
        dy, dg = (step // (z_size * x_size)) % y_size, step // (z_size * x_size * y_size)
        to = (((y + dy) % y_size) * z_size + (z + dz) % z_size) * x_size + (x + dx) % x_size
        return to, (g + dg) % g_size

    barrier = pltpu.get_barrier_semaphore()

    @pl.loop(1, devices)
    def _(step):
        pl.semaphore_signal(barrier, inc=1, device_id=peer(step), device_id_type=MESH)

    for load in loads:
        load.wait()

    group = LANES // 8
    span = group * col_width

    @pl.loop(0, width // span)
    def _(chunk):
        lanes = pl.ds(pl.multiple_of(chunk * span, LANES), span)
        parts = []
        for layer in range(layers):
            for block in range(rows // BLOCK):
                scale = jnp.exp2(exps[layer, block : block + 1, lanes].astype(jnp.float32))
                value = codes[layer, block * BLOCK : (block + 1) * BLOCK, lanes].astype(jnp.float32)
                parts.append(value * scale)
        blocks = jnp.concatenate(parts, axis=0).T.reshape(group, col_width, layers * rows)
        turned[pl.ds(chunk * group, group)] = blocks

    @pl.loop(0, devices)
    def _(to):
        send[to] = turned[cmap[to]].astype(send.dtype)

    pl.semaphore_wait(barrier, devices - 1)

    @pl.loop(1, devices)
    def _(step):
        to, to_g = peer(step)
        pltpu.make_async_remote_copy(
            src_ref=send.at[to * g_size + to_g],
            dst_ref=recv.at[me],
            send_sem=send_sem,
            recv_sem=recv_sem,
            device_id=(to, to_g),
            device_id_type=MESH,
        ).start()

    own = pltpu.make_async_copy(send.at[me], recv.at[me], own_sem)
    own.start()
    own.wait()
    others = pl.ds(0, devices - 1)
    pltpu.make_async_copy(recv.at[others], recv.at[others], recv_sem).wait()
    pltpu.make_async_copy(send.at[others], send.at[others], send_sem).wait()


def assemble(order, recv, rollout, sums):
    layers, col_width, span = rollout.shape
    half = LANES // layers
    first = pl.program_id(0) * (span // half)
    low = lax.broadcasted_iota(jnp.int32, (col_width, LANES), 1) < half
    group = 2 * LANES
    totals = [jnp.zeros((col_width, LANES), jnp.float32) for _ in range(layers)]
    row = lax.broadcasted_iota(jnp.int32, (group, LANES), 0) // BLOCK
    lane = lax.broadcasted_iota(jnp.int32, (group, LANES), 1)
    for at in range(0, span, group):
        tiles = [[] for _ in range(layers)]
        for pair in range(at, at + group, LANES):
            k = first + pair // half
            a, b = recv[order[k]], recv[order[k + 1]]
            tiles[0].append(jnp.concatenate([a[:, :half], b[:, :half]], axis=1))
            tiles[1].append(jnp.concatenate([a[:, half:], b[:, half:]], axis=1))
        picks = (row + at // BLOCK == lane).astype(jnp.bfloat16)
        for layer in range(layers):
            both = jnp.concatenate(tiles[layer], axis=1)
            rollout[layer, :, at : at + group] = both
            totals[layer] += jnp.dot(both, picks, preferred_element_type=jnp.float32)
    for layer in range(layers):
        sums[layer] = totals[layer]


def shards(sizes, codes, exponents, column_map, row_order):
    layers, rows, width = codes.shape
    devices = sizes[0] * sizes[1] * sizes[2] * sizes[3]
    col_width = width // devices
    anywhere = pl.BlockSpec(memory_space=pl.ANY)
    landed = pl.pallas_call(
        functools.partial(exchange, sizes),
        out_shape=jax.ShapeDtypeStruct((devices, col_width, layers * rows), jnp.bfloat16),
        in_specs=[anywhere] * 3,
        out_specs=anywhere,
        scratch_shapes=[
            pltpu.VMEM(codes.shape, codes.dtype),
            pltpu.VMEM(exponents.shape, exponents.dtype),
            pltpu.SMEM(column_map.shape, column_map.dtype),
            pltpu.VMEM((devices, col_width, layers * rows), jnp.float32),
            pltpu.VMEM((devices, col_width, layers * rows), jnp.bfloat16),
            pltpu.SemaphoreType.DMA((3,)),
            pltpu.SemaphoreType.DMA(()),
            pltpu.SemaphoreType.DMA(()),
            pltpu.SemaphoreType.DMA(()),
        ],
        compiler_params=pltpu.CompilerParams(
            collective_id=0, has_side_effects=True, vmem_limit_bytes=16 << 20
        ),
        name="exchange",
    )(codes, exponents, column_map)
    span = LANES * BLOCK
    return pl.pallas_call(
        assemble,
        grid=(devices * rows // span,),
        out_shape=(
            jax.ShapeDtypeStruct((layers, col_width, devices * rows), jnp.bfloat16),
            jax.ShapeDtypeStruct((layers, col_width, devices * rows // BLOCK), jnp.float32),
        ),
        in_specs=[
            pl.BlockSpec(memory_space=pltpu.SMEM),
            pl.BlockSpec(memory_space=pltpu.VMEM),
        ],
        out_specs=(
            pl.BlockSpec((layers, col_width, span), lambda i: (0, 0, i)),
            pl.BlockSpec((layers, col_width, LANES), lambda i: (0, 0, i)),
        ),
        compiler_params=pltpu.CompilerParams(vmem_limit_bytes=16 << 20),
        name="assemble",
    )(row_order, landed)


def solution(mesh):
    chain, grp = mesh.shape["chain"], mesh.shape["grp"]
    z_size = next(n for n in range(1, chain + 1) if n ** 3 >= 4 * chain)
    side = 1
    while side * side * z_size < chain:
        side += 1
    sizes = (side, side, z_size, grp)
    assert side * side * z_size == chain
    return jax.shard_map(
        functools.partial(shards, sizes),
        mesh=mesh,
        in_specs=(P(None, ("chain", "grp"), None), P(None, ("chain", "grp"), None), P(), P()),
        out_specs=(P(None, ("chain", "grp"), None), P(None, ("chain", "grp"), None)),
        check_vma=False,
    )
```

```python
import functools

import jax
import jax.numpy as jnp
from jax import lax
from jax.experimental import pallas as pl
from jax.experimental.pallas import tpu as pltpu
from jax.sharding import PartitionSpec as P

MESH = pl.DeviceIdType.MESH
BLOCK = 32
LANES = 128


def hops(d, size):
    return min(d, size - d)


def plan(sizes):
    x_size, y_size, z_size, g_size = sizes

    def distance(o):
        return hops(o[0], x_size) + hops(o[1], y_size) + hops(o[2], z_size)

    offsets = [
        (dx, dy, dz, dg)
        for dg in range(g_size)
        for dy in range(y_size)
        for dx in range(x_size)
        for dz in range(z_size)
    ][1:]
    reach = hops(x_size // 2, x_size) + hops(y_size // 2, y_size)
    reach = max(reach, hops(z_size // 2, z_size))
    middles = [(0, 0, z_size // 2, 0), (x_size // 2, y_size // 2, 0, 0)]
    ordered = []
    for o in sorted(offsets, key=lambda o: -distance(o)):
        back = (-o[0] % x_size, -o[1] % y_size, -o[2] % z_size)
        for twin in (o[:3], back):
            for dg in range(g_size):
                if twin + (dg,) in offsets and twin + (dg,) not in ordered:
                    ordered.append(twin + (dg,))
    near = [o for o in ordered if distance(o) <= reach]
    far = [o for o in ordered if distance(o) > reach]
    for o in far:
        gaps = [tuple((p - q) % n for p, q, n in zip(o, m, sizes)) for m in middles]
        assert any(distance(gap) <= reach for gap in gaps)
    return near, far, [m for m in middles if m in near]


def exchange(sizes, codes_hbm, exps_hbm, cmap_hbm, recv, codes, exps, cmap, turned, send, load_sem, send_sem, recv_sem, mid_sem):
    x_size, y_size, z_size, g_size = sizes
    devices = x_size * y_size * z_size * g_size
    layers, rows, width = codes.shape
    col_width = width // devices
    near, far, middles = plan(sizes)

    loads = [
        pltpu.make_async_copy(codes_hbm, codes, load_sem.at[0]),
        pltpu.make_async_copy(exps_hbm, exps, load_sem.at[1]),
        pltpu.make_async_copy(cmap_hbm, cmap, load_sem.at[2]),
    ]
    for load in loads:
        load.start()

    chain, g = lax.axis_index("chain"), lax.axis_index("grp")
    x, z, y = lax.rem(chain, x_size), lax.rem(lax.div(chain, x_size), z_size), lax.div(chain, x_size * z_size)
    me = chain * g_size + g
    across = [lax.rem(x + d, x_size) for d in range(x_size)]
    along = [lax.rem(z + d, z_size) * x_size for d in range(z_size)]
    down = [lax.rem(y + d, y_size) * (x_size * z_size) for d in range(y_size)]
    cores = [lax.rem(g + d, g_size) for d in range(g_size)]
    planes = {(dx, dy): down[dy] + across[dx] for dx in range(x_size) for dy in range(y_size)}

    def peer(o):
        return planes[o[:2]] + along[o[2]], cores[o[3]]

    barrier = pltpu.get_barrier_semaphore()
    for o in near:
        pl.semaphore_signal(barrier, inc=1, device_id=peer(o), device_id_type=MESH)

    for load in loads:
        load.wait()

    group = LANES // 8
    span = group * col_width

    @pl.loop(0, width // span)
    def _(chunk):
        lanes = pl.ds(pl.multiple_of(chunk * span, LANES), span)
        parts = []
        for layer in range(layers):
            for block in range(rows // BLOCK):
                scale = jnp.exp2(exps[layer, block : block + 1, lanes].astype(jnp.float32))
                value = codes[layer, block * BLOCK : (block + 1) * BLOCK, lanes].astype(jnp.float32)
                parts.append(value * scale)
        blocks = jnp.concatenate(parts, axis=0).T.reshape(group, col_width, layers * rows)
        turned[pl.ds(chunk * group, group)] = blocks

    def gather(slot, o):
        to, to_g = peer(o)
        send[slot] = turned[cmap[to * g_size + to_g]].astype(send.dtype)

    def launch(slot, o):
        pltpu.make_async_remote_copy(
            src_ref=send.at[slot],
            dst_ref=recv.at[me],
            send_sem=send_sem,
            recv_sem=recv_sem,
            device_id=peer(o),
            device_id_type=MESH,
        ).start()

    recv[me] = turned[cmap[me]].astype(recv.dtype)
    for slot, o in enumerate(near + far):
        gather(slot, o)

    pl.semaphore_wait(barrier, len(near))
    for m in middles:
        pl.semaphore_signal(mid_sem, inc=1, device_id=peer(m), device_id_type=MESH)
    for slot, o in enumerate(near):
        launch(slot, o)
    pl.semaphore_wait(mid_sem, len(middles))
    for slot, o in enumerate(far):
        launch(len(near) + slot, o)
    others = recv.at[pl.ds(0, devices - 1)]
    pltpu.make_async_copy(others, others, recv_sem).wait()
    pltpu.make_async_copy(send, send, send_sem).wait()


def assemble(order, recv, rollout, sums):
    layers, col_width, span = rollout.shape
    half = LANES // layers
    first = pl.program_id(0) * (span // half)
    low = lax.broadcasted_iota(jnp.int32, (col_width, LANES), 1) < half
    group = 2 * LANES
    totals = [jnp.zeros((col_width, LANES), jnp.float32) for _ in range(layers)]
    row = lax.broadcasted_iota(jnp.int32, (group, LANES), 0) // BLOCK
    lane = lax.broadcasted_iota(jnp.int32, (group, LANES), 1)
    for at in range(0, span, group):
        tiles = [[] for _ in range(layers)]
        for pair in range(at, at + group, LANES):
            k = first + pair // half
            a, b = recv[order[k]], recv[order[k + 1]]
            tiles[0].append(jnp.concatenate([a[:, :half], b[:, :half]], axis=1))
            tiles[1].append(jnp.concatenate([a[:, half:], b[:, half:]], axis=1))
        picks = (row + at // BLOCK == lane).astype(jnp.bfloat16)
        for layer in range(layers):
            both = jnp.concatenate(tiles[layer], axis=1)
            rollout[layer, :, at : at + group] = both
            totals[layer] += jnp.dot(both, picks, preferred_element_type=jnp.float32)
    for layer in range(layers):
        sums[layer] = totals[layer]


def shards(sizes, codes, exponents, column_map, row_order):
    layers, rows, width = codes.shape
    devices = sizes[0] * sizes[1] * sizes[2] * sizes[3]
    col_width = width // devices
    anywhere = pl.BlockSpec(memory_space=pl.ANY)
    landed = pl.pallas_call(
        functools.partial(exchange, sizes),
        out_shape=pltpu.VMEM((devices, col_width, layers * rows), jnp.bfloat16),
        in_specs=[anywhere] * 3,
        out_specs=pl.BlockSpec(memory_space=pltpu.VMEM),
        scratch_shapes=[
            pltpu.VMEM(codes.shape, codes.dtype),
            pltpu.VMEM(exponents.shape, exponents.dtype),
            pltpu.SMEM(column_map.shape, column_map.dtype),
            pltpu.VMEM((devices, col_width, layers * rows), jnp.float32),
            pltpu.VMEM((devices - 1, col_width, layers * rows), jnp.bfloat16),
            pltpu.SemaphoreType.DMA((3,)),
            pltpu.SemaphoreType.DMA(()),
            pltpu.SemaphoreType.DMA(()),
            pltpu.SemaphoreType.REGULAR,
        ],
        compiler_params=pltpu.CompilerParams(
            collective_id=0, has_side_effects=True, vmem_limit_bytes=60 << 20
        ),
        name="exchange",
    )(codes, exponents, column_map)
    span = LANES * BLOCK
    return pl.pallas_call(
        assemble,
        grid=(devices * rows // span,),
        out_shape=(
            jax.ShapeDtypeStruct((layers, col_width, devices * rows), jnp.bfloat16),
            jax.ShapeDtypeStruct((layers, col_width, devices * rows // BLOCK), jnp.float32),
        ),
        in_specs=[
            pl.BlockSpec(memory_space=pltpu.SMEM),
            pl.BlockSpec(memory_space=pltpu.VMEM),
        ],
        out_specs=(
            pl.BlockSpec((layers, col_width, span), lambda i: (0, 0, i)),
            pl.BlockSpec((layers, col_width, LANES), lambda i: (0, 0, i)),
        ),
        compiler_params=pltpu.CompilerParams(vmem_limit_bytes=16 << 20),
        name="assemble",
    )(row_order, landed)


def solution(mesh):
    chain, grp = mesh.shape["chain"], mesh.shape["grp"]
    z_size = next(n for n in range(1, chain + 1) if n ** 3 >= 4 * chain)
    side = 1
    while side * side * z_size < chain:
        side += 1
    sizes = (side, side, z_size, grp)
    assert side * side * z_size == chain
    return jax.shard_map(
        functools.partial(shards, sizes),
        mesh=mesh,
        in_specs=(P(None, ("chain", "grp"), None), P(None, ("chain", "grp"), None), P(), P()),
        out_specs=(P(None, ("chain", "grp"), None), P(None, ("chain", "grp"), None)),
        check_vma=False,
    )
```

```python
import functools

import jax
import jax.numpy as jnp
from jax import lax
from jax.experimental import pallas as pl
from jax.experimental.pallas import tpu as pltpu
from jax.sharding import PartitionSpec as P

MESH = pl.DeviceIdType.MESH
BLOCK = 32
LANES = 128


def hops(d, size):
    return min(d, size - d)


def plan(sizes):
    x_size, y_size, z_size, g_size = sizes

    def distance(o):
        return hops(o[0], x_size) + hops(o[1], y_size) + hops(o[2], z_size)

    offsets = [
        (dx, dy, dz, dg)
        for dg in range(g_size)
        for dy in range(y_size)
        for dx in range(x_size)
        for dz in range(z_size)
    ][1:]
    reach = hops(x_size // 2, x_size) + hops(y_size // 2, y_size)
    reach = max(reach, hops(z_size // 2, z_size))
    middles = [(0, 0, z_size // 2, 0), (x_size // 2, y_size // 2, 0, 0)]
    ordered = []
    for o in sorted(offsets, key=lambda o: -distance(o)):
        back = (-o[0] % x_size, -o[1] % y_size, -o[2] % z_size)
        for twin in (o[:3], back):
            for dg in range(g_size):
                if twin + (dg,) in offsets and twin + (dg,) not in ordered:
                    ordered.append(twin + (dg,))
    near = [o for o in ordered if distance(o) <= reach]
    far = [o for o in ordered if distance(o) > reach]
    for o in far:
        gaps = [tuple((p - q) % n for p, q, n in zip(o, m, sizes)) for m in middles]
        assert any(distance(gap) <= reach for gap in gaps)
    return near, far, [m for m in middles if m in near]


def exchange(sizes, codes_hbm, exps_hbm, cmap_hbm, recv, codes, exps, cmap, turned, send, load_sem, send_sem, recv_sem, mid_sem):
    x_size, y_size, z_size, g_size = sizes
    devices = x_size * y_size * z_size * g_size
    layers, rows, width = codes.shape
    col_width = width // devices
    near, far, middles = plan(sizes)

    pieces = 2
    piece = width // pieces
    load_exps = pltpu.make_async_copy(exps_hbm, exps, load_sem.at[pieces])
    load_exps.start()
    loads = []
    for i in range(pieces):
        lanes = pl.ds(i * piece, piece)
        loads.append(pltpu.make_async_copy(codes_hbm.at[:, :, lanes], codes.at[:, :, lanes], load_sem.at[i]))
        loads[-1].start()
    load_cmap = pltpu.make_async_copy(cmap_hbm, cmap, load_sem.at[pieces + 1])
    load_cmap.start()

    chain, g = lax.axis_index("chain"), lax.axis_index("grp")
    x, z, y = lax.rem(chain, x_size), lax.rem(lax.div(chain, x_size), z_size), lax.div(chain, x_size * z_size)
    me = chain * g_size + g
    across = [lax.rem(x + d, x_size) for d in range(x_size)]
    along = [lax.rem(z + d, z_size) * x_size for d in range(z_size)]
    down = [lax.rem(y + d, y_size) * (x_size * z_size) for d in range(y_size)]
    cores = [lax.rem(g + d, g_size) for d in range(g_size)]
    planes = {(dx, dy): down[dy] + across[dx] for dx in range(x_size) for dy in range(y_size)}

    def peer(o):
        return planes[o[:2]] + along[o[2]], cores[o[3]]

    barrier = pltpu.get_barrier_semaphore()
    for o in near:
        pl.semaphore_signal(barrier, inc=1, device_id=peer(o), device_id_type=MESH)

    load_exps.wait()
    group = LANES // 8
    span = group * col_width
    for chunk in range(width // span):
        if chunk * span % piece == 0:
            loads[chunk * span // piece].wait()
        lanes = pl.ds(chunk * span, span)
        parts = []
        for layer in range(layers):
            for block in range(rows // BLOCK):
                scale = jnp.exp2(exps[layer, block : block + 1, lanes].astype(jnp.float32))
                part = codes[layer, block * BLOCK : (block + 1) * BLOCK, lanes]
                parts.append(part * scale.astype(part.dtype))
        blocks = jnp.concatenate(parts, axis=0).T.reshape(group, col_width, layers * rows)
        turned[pl.ds(chunk * group, group)] = blocks
    load_cmap.wait()

    def gather(slot, o):
        to, to_g = peer(o)
        send[slot] = turned[cmap[to * g_size + to_g]]

    def launch(slot, o):
        pltpu.make_async_remote_copy(
            src_ref=send.at[slot],
            dst_ref=recv.at[me],
            send_sem=send_sem,
            recv_sem=recv_sem,
            device_id=peer(o),
            device_id_type=MESH,
        ).start()

    recv[me] = turned[cmap[me]]
    for slot, o in enumerate(near + far):
        gather(slot, o)

    pl.semaphore_wait(barrier, len(near))
    for m in middles:
        pl.semaphore_signal(mid_sem, inc=1, device_id=peer(m), device_id_type=MESH)
    for slot, o in enumerate(near):
        launch(slot, o)
    pl.semaphore_wait(mid_sem, len(middles))
    for slot, o in enumerate(far):
        launch(len(near) + slot, o)
    others = recv.at[pl.ds(0, devices - 1)]
    pltpu.make_async_copy(others, others, recv_sem).wait()
    pltpu.make_async_copy(send, send, send_sem).wait()


def assemble(order, recv, rollout, sums, tiles, totals, out_sem):
    layers, col_width, width = rollout.shape
    half = LANES // layers
    quad = 2 * LANES
    span = LANES * BLOCK
    part = span // 2
    lane = lax.broadcasted_iota(jnp.int32, (col_width, LANES), 1)
    low = lane < half
    sources = lax.broadcasted_iota(jnp.int32, (quad, LANES), 0) // BLOCK
    targets = lax.broadcasted_iota(jnp.int32, (quad, LANES), 1) % (quad // BLOCK)
    picks = (sources == targets).astype(jnp.bfloat16)
    copies = []
    for at in range(0, width, LANES):
        k = at // half
        a, b = recv[order[k]], recv[order[k + 1]]
        crossed = pltpu.roll(jnp.where(low, b, a), half, 1)
        tiles[0, :, at : at + LANES] = jnp.where(low, a, crossed)
        tiles[1, :, at : at + LANES] = jnp.where(low, crossed, b)
        done = at + LANES
        if done % part == 0:
            lanes = pl.ds(done - part, part)
            copies.append(pltpu.make_async_copy(tiles.at[:, :, lanes], rollout.at[:, :, lanes], out_sem.at[done // part - 1]))
            copies[-1].start()
    for start in range(0, width, span):
        for layer in range(layers):
            stacked = jnp.concatenate(
                [tiles[layer, :, at : at + quad] for at in range(start, start + span, quad)], axis=0
            )
            got = jnp.dot(stacked, picks, preferred_element_type=jnp.float32)
            got = got.reshape(span // quad, col_width, LANES)
            total = got[0]
            for i in range(1, span // quad):
                total = jnp.where(lane // (quad // BLOCK) == i, got[i], total)
            totals[layer, :, start // BLOCK : start // BLOCK + LANES] = total
    copies.append(pltpu.make_async_copy(totals, sums, out_sem.at[width // part]))
    copies[-1].start()
    for copy in copies:
        copy.wait()


def shards(sizes, codes, exponents, column_map, row_order):
    layers, rows, width = codes.shape
    devices = sizes[0] * sizes[1] * sizes[2] * sizes[3]
    col_width = width // devices
    anywhere = pl.BlockSpec(memory_space=pl.ANY)
    landed = pl.pallas_call(
        functools.partial(exchange, sizes),
        out_shape=pltpu.VMEM((devices, col_width, layers * rows), jnp.bfloat16),
        in_specs=[anywhere] * 3,
        out_specs=pl.BlockSpec(memory_space=pltpu.VMEM),
        scratch_shapes=[
            pltpu.VMEM(codes.shape, codes.dtype),
            pltpu.VMEM(exponents.shape, exponents.dtype),
            pltpu.SMEM(column_map.shape, column_map.dtype),
            pltpu.VMEM((devices, col_width, layers * rows), codes.dtype),
            pltpu.VMEM((devices - 1, col_width, layers * rows), jnp.bfloat16),
            pltpu.SemaphoreType.DMA((4,)),
            pltpu.SemaphoreType.DMA(()),
            pltpu.SemaphoreType.DMA(()),
            pltpu.SemaphoreType.REGULAR,
        ],
        compiler_params=pltpu.CompilerParams(
            collective_id=0, has_side_effects=True, vmem_limit_bytes=60 << 20
        ),
        name="exchange",
    )(codes, exponents, column_map)
    rollout = jax.ShapeDtypeStruct((layers, col_width, devices * rows), jnp.bfloat16)
    sums = jax.ShapeDtypeStruct((layers, col_width, devices * rows // BLOCK), jnp.float32)
    return pl.pallas_call(
        assemble,
        out_shape=(rollout, sums),
        in_specs=[
            pl.BlockSpec(memory_space=pltpu.SMEM),
            pl.BlockSpec(memory_space=pltpu.VMEM),
        ],
        out_specs=(anywhere, anywhere),
        scratch_shapes=[
            pltpu.VMEM(rollout.shape, rollout.dtype),
            pltpu.VMEM(sums.shape, sums.dtype),
            pltpu.SemaphoreType.DMA((9,)),
        ],
        compiler_params=pltpu.CompilerParams(vmem_limit_bytes=16 << 20),
        name="assemble",
    )(row_order, landed)


def solution(mesh):
    chain, grp = mesh.shape["chain"], mesh.shape["grp"]
    z_size = next(n for n in range(1, chain + 1) if n ** 3 >= 4 * chain)
    side = 1
    while side * side * z_size < chain:
        side += 1
    sizes = (side, side, z_size, grp)
    assert side * side * z_size == chain
    return jax.shard_map(
        functools.partial(shards, sizes),
        mesh=mesh,
        in_specs=(P(None, ("chain", "grp"), None), P(None, ("chain", "grp"), None), P(), P()),
        out_specs=(P(None, ("chain", "grp"), None), P(None, ("chain", "grp"), None)),
        check_vma=False,
    )
```

```python
import functools

import jax
import jax.numpy as jnp
from jax import lax
from jax.experimental import pallas as pl
from jax.experimental.pallas import tpu as pltpu
from jax.sharding import PartitionSpec as P

MESH = pl.DeviceIdType.MESH
BLOCK = 32
LANES = 128


def hops(d, size):
    return min(d, size - d)


def plan(sizes):
    x_size, y_size, z_size, g_size = sizes
    offsets = [
        (dx, dy, dz, dg)
        for dg in range(g_size)
        for dy in range(y_size)
        for dx in range(x_size)
        for dz in range(z_size)
    ]

    def distance(o):
        return hops(o[0], x_size) + hops(o[1], y_size) + hops(o[2], z_size)

    greeted = [o for o in offsets[1:] if o[:2] == (0, 0) or o[2] == 0]
    greeted = sorted(greeted, key=lambda o: -distance(o))
    column = [o for o in offsets[1:] if o[:2] == (0, 0)]
    place = {
        o + (0,): i / len(offsets)
        + 0.07 * (o[0] >= x_size // 2) + 0.1 * (o[1] >= y_size // 2) + 0.3 * (o[2] >= z_size // 2)
        for i, o in enumerate(offsets)
    }
    return greeted, column, sorted(place, key=lambda o: place[o])


def exchange(sizes, codes_hbm, exps_hbm, cmap_hbm, recv, codes, exps, cmap, turned, send, load_sem, send_sem, recv_sem, line_sem):
    x_size, y_size, z_size, g_size = sizes
    devices = x_size * y_size * z_size * g_size
    layers, rows, width = codes.shape
    col_width = width // devices
    greeted, column, rest = plan(sizes)

    chain, g = lax.axis_index("chain"), lax.axis_index("grp")
    x, z = lax.rem(chain, x_size), lax.rem(lax.div(chain, x_size), z_size)
    y = lax.div(chain, x_size * z_size)
    me = chain * g_size + g
    cores = [lax.rem(g + d, g_size) for d in range(g_size)]

    def relative(at, size, step):
        return [lax.rem(at + d, size) * step for d in range(size)]

    def halved(at, size, step):
        half = size // 2
        turn = lax.rem(at, half)
        return [(h * half + lax.rem(turn + i, half)) * step for h in range(2) for i in range(half)]

    steps = ((x, x_size, 1), (y, y_size, x_size * z_size), (z, z_size, x_size))
    near_x, near_y, near_z = (relative(*s) for s in steps)
    all_x, all_y, all_z = (halved(*s) for s in steps)

    def peer(o):
        if len(o) == 4:
            return near_y[o[1]] + near_x[o[0]] + near_z[o[2]], cores[o[3]]
        return all_y[o[1]] + all_x[o[0]] + all_z[o[2]], cores[o[3]]

    barrier = pltpu.get_barrier_semaphore()
    for o in greeted:
        pl.semaphore_signal(barrier, inc=1, device_id=peer(o), device_id_type=MESH)

    pieces = 2
    piece = width // pieces
    load_exps = pltpu.make_async_copy(exps_hbm, exps, load_sem.at[pieces])
    load_exps.start()
    loads = []
    for i in range(pieces):
        lanes = pl.ds(i * piece, piece)
        loads.append(pltpu.make_async_copy(codes_hbm.at[:, :, lanes], codes.at[:, :, lanes], load_sem.at[i]))
        loads[-1].start()
    load_cmap = pltpu.make_async_copy(cmap_hbm, cmap, load_sem.at[pieces + 1])
    load_cmap.start()

    load_exps.wait()
    group = LANES // 8
    span = group * col_width
    for chunk in range(width // span):
        if chunk * span % piece == 0:
            loads[chunk * span // piece].wait()
        lanes = pl.ds(chunk * span, span)
        parts = []
        for layer in range(layers):
            for block in range(rows // BLOCK):
                scale = jnp.exp2(exps[layer, block : block + 1, lanes].astype(jnp.float32))
                part = codes[layer, block * BLOCK : (block + 1) * BLOCK, lanes]
                parts.append(part * scale.astype(part.dtype))
        blocks = jnp.concatenate(parts, axis=0).T.reshape(group, col_width, layers * rows)
        turned[pl.ds(chunk * group, group)] = blocks
    load_cmap.wait()

    def gather(slot, o):
        to, to_g = peer(o)
        send[slot] = turned[cmap[to * g_size + to_g]]

    def copy(slot, o):
        return pltpu.make_async_remote_copy(
            src_ref=send.at[slot],
            dst_ref=recv.at[me],
            send_sem=send_sem,
            recv_sem=recv_sem,
            device_id=peer(o),
            device_id_type=MESH,
        )

    recv[me] = turned[cmap[me]]
    for slot, o in enumerate(column + rest):
        gather(slot, o)

    pl.semaphore_wait(barrier, len(greeted))
    line = [(0, 0, d, 0) for d in range(1, z_size)]
    for o in sorted(line, key=lambda o: -hops(o[2], z_size)):
        pl.semaphore_signal(line_sem, inc=1, device_id=peer(o), device_id_type=MESH)
    for slot, o in enumerate(column):
        copy(slot, o).start()
    pl.semaphore_wait(line_sem, len(line))
    for slot, o in enumerate(rest):
        here = (all_x[o[0]] == x).astype(jnp.int32) + (all_y[o[1]] == near_y[0]).astype(jnp.int32)
        pl.when(here < 2)(copy(len(column) + slot, o).start)

    others = recv.at[pl.ds(0, devices - 1)]
    pltpu.make_async_copy(others, others, recv_sem).wait()
    pltpu.make_async_copy(others, others, send_sem).wait()


def assemble(order, recv, rollout, sums, tiles, totals, out_sem):
    layers, col_width, width = rollout.shape
    half = LANES // layers
    quad = 2 * LANES
    span = LANES * BLOCK
    part = span // 2
    lane = lax.broadcasted_iota(jnp.int32, (col_width, LANES), 1)
    low = lane < half
    sources = lax.broadcasted_iota(jnp.int32, (quad, LANES), 0) // BLOCK
    targets = lax.broadcasted_iota(jnp.int32, (quad, LANES), 1) % (quad // BLOCK)
    picks = (sources == targets).astype(jnp.bfloat16)
    copies = []
    for at in range(0, width, LANES):
        k = at // half
        a, b = recv[order[k]], recv[order[k + 1]]
        crossed = pltpu.roll(jnp.where(low, b, a), half, 1)
        tiles[0, :, at : at + LANES] = jnp.where(low, a, crossed)
        tiles[1, :, at : at + LANES] = jnp.where(low, crossed, b)
        done = at + LANES
        if done % part == 0:
            lanes = pl.ds(done - part, part)
            copies.append(pltpu.make_async_copy(tiles.at[:, :, lanes], rollout.at[:, :, lanes], out_sem.at[done // part - 1]))
            copies[-1].start()
    for start in range(0, width, span):
        for layer in range(layers):
            stacked = jnp.concatenate(
                [tiles[layer, :, at : at + quad] for at in range(start, start + span, quad)], axis=0
            )
            got = jnp.dot(stacked, picks, preferred_element_type=jnp.float32)
            got = got.reshape(span // quad, col_width, LANES)
            total = got[0]
            for i in range(1, span // quad):
                total = jnp.where(lane // (quad // BLOCK) == i, got[i], total)
            totals[layer, :, start // BLOCK : start // BLOCK + LANES] = total
    copies.append(pltpu.make_async_copy(totals, sums, out_sem.at[width // part]))
    copies[-1].start()
    for copy in copies:
        copy.wait()


def shards(sizes, codes, exponents, column_map, row_order):
    layers, rows, width = codes.shape
    devices = sizes[0] * sizes[1] * sizes[2] * sizes[3]
    column = sizes[2] * sizes[3]
    col_width = width // devices
    anywhere = pl.BlockSpec(memory_space=pl.ANY)
    landed = pl.pallas_call(
        functools.partial(exchange, sizes),
        out_shape=pltpu.VMEM((devices, col_width, layers * rows), jnp.bfloat16),
        in_specs=[anywhere] * 3,
        out_specs=pl.BlockSpec(memory_space=pltpu.VMEM),
        scratch_shapes=[
            pltpu.VMEM(codes.shape, codes.dtype),
            pltpu.VMEM(exponents.shape, exponents.dtype),
            pltpu.SMEM(column_map.shape, column_map.dtype),
            pltpu.VMEM((devices, col_width, layers * rows), codes.dtype),
            pltpu.VMEM((devices + column - 1, col_width, layers * rows), jnp.bfloat16),
            pltpu.SemaphoreType.DMA((4,)),
            pltpu.SemaphoreType.DMA(()),
            pltpu.SemaphoreType.DMA(()),
            pltpu.SemaphoreType.REGULAR,
        ],
        compiler_params=pltpu.CompilerParams(
            collective_id=0, has_side_effects=True, vmem_limit_bytes=60 << 20
        ),
        name="exchange",
    )(codes, exponents, column_map)
    rollout = jax.ShapeDtypeStruct((layers, col_width, devices * rows), jnp.bfloat16)
    sums = jax.ShapeDtypeStruct((layers, col_width, devices * rows // BLOCK), jnp.float32)
    return pl.pallas_call(
        assemble,
        out_shape=(rollout, sums),
        in_specs=[
            pl.BlockSpec(memory_space=pltpu.SMEM),
            pl.BlockSpec(memory_space=pltpu.VMEM),
        ],
        out_specs=(anywhere, anywhere),
        scratch_shapes=[
            pltpu.VMEM(rollout.shape, rollout.dtype),
            pltpu.VMEM(sums.shape, sums.dtype),
            pltpu.SemaphoreType.DMA((9,)),
        ],
        compiler_params=pltpu.CompilerParams(vmem_limit_bytes=16 << 20),
        name="assemble",
    )(row_order, landed)


def solution(mesh):
    chain, grp = mesh.shape["chain"], mesh.shape["grp"]
    z_size = next(n for n in range(1, chain + 1) if n ** 3 >= 4 * chain)
    side = 1
    while side * side * z_size < chain:
        side += 1
    sizes = (side, side, z_size, grp)
    assert side * side * z_size == chain
    return jax.shard_map(
        functools.partial(shards, sizes),
        mesh=mesh,
        in_specs=(P(None, ("chain", "grp"), None), P(None, ("chain", "grp"), None), P(), P()),
        out_specs=(P(None, ("chain", "grp"), None), P(None, ("chain", "grp"), None)),
        check_vma=False,
    )
```

```python
import functools

import jax
import jax.numpy as jnp
from jax import lax
from jax.experimental import pallas as pl
from jax.experimental.pallas import tpu as pltpu
from jax.sharding import PartitionSpec as P

MESH = pl.DeviceIdType.MESH
BLOCK = 32
LANES = 128


def hops(d, size):
    return min(d, size - d)


def plan(sizes):
    x_size, y_size, z_size, g_size = sizes
    offsets = [
        (dx, dy, dz, dg)
        for dg in range(g_size)
        for dy in range(y_size)
        for dx in range(x_size)
        for dz in range(z_size)
    ]

    def distance(o):
        return hops(o[0], x_size) + hops(o[1], y_size) + hops(o[2], z_size)

    greeted = [o for o in offsets[1:] if o[:2] == (0, 0) or o[2] == 0]
    greeted = sorted(greeted, key=lambda o: -distance(o))
    column = [o for o in offsets[1:] if o[:2] == (0, 0)]
    base = sorted(offsets, key=lambda o: ([0,2,1,3][o[1]],o[0],o[3],o[2]))
    place = {
        o + (0,): i / len(offsets)
        + 0.07 * (o[0] >= x_size // 2) + 0.2 * (o[1] >= y_size // 2) + 0.3 * (o[2] >= z_size // 2)
        for i, o in enumerate(base)
    }
    return greeted, column, sorted(place, key=lambda o: place[o])


def exchange(sizes, codes_hbm, exps_hbm, cmap_hbm, order_hbm, tiles, codes, exps, cmap, order, turned, send, recv, load_sem, send_sem, recv_sem, line_sem):
    x_size, y_size, z_size, g_size = sizes
    devices = x_size * y_size * z_size * g_size
    layers, rows, width = codes.shape
    col_width = width // devices
    greeted, column, rest = plan(sizes)

    chain, g = lax.axis_index("chain"), lax.axis_index("grp")
    x, z = lax.rem(chain, x_size), lax.rem(lax.div(chain, x_size), z_size)
    y = lax.div(chain, x_size * z_size)
    me = chain * g_size + g
    cores = [lax.rem(g + d, g_size) for d in range(g_size)]

    def relative(at, size, step):
        return [lax.rem(at + d, size) * step for d in range(size)]

    def halved(at, size, step):
        half = size // 2
        turn = lax.rem(at, half)
        return [(h * half + lax.rem(turn + i, half)) * step for h in range(2) for i in range(half)]

    steps = ((x, x_size, 1), (y, y_size, x_size * z_size), (z, z_size, x_size))
    near_x, near_y, near_z = (relative(*s) for s in steps)
    all_x, all_y, all_z = (halved(*s) for s in steps)

    def peer(o):
        if len(o) == 4:
            return near_y[o[1]] + near_x[o[0]] + near_z[o[2]], cores[o[3]]
        return all_y[o[1]] + all_x[o[0]] + all_z[o[2]], cores[o[3]]

    barrier = pltpu.get_barrier_semaphore()
    for o in greeted:
        pl.semaphore_signal(barrier, inc=1, device_id=peer(o), device_id_type=MESH)

    pieces = 2
    piece = width // pieces
    load_exps = pltpu.make_async_copy(exps_hbm, exps, load_sem.at[pieces])
    load_exps.start()
    loads = []
    for i in range(pieces):
        lanes = pl.ds(i * piece, piece)
        loads.append(pltpu.make_async_copy(codes_hbm.at[:, :, lanes], codes.at[:, :, lanes], load_sem.at[i]))
        loads[-1].start()
    load_cmap = pltpu.make_async_copy(cmap_hbm, cmap, load_sem.at[pieces + 1])
    load_cmap.start()
    load_order = pltpu.make_async_copy(order_hbm, order, load_sem.at[pieces + 2])
    load_order.start()

    load_exps.wait()
    group = LANES // 8
    span = group * col_width
    for chunk in range(width // span):
        if chunk * span % piece == 0:
            loads[chunk * span // piece].wait()
        lanes = pl.ds(chunk * span, span)
        parts = []
        for layer in range(layers):
            for block in range(rows // BLOCK):
                scale = jnp.exp2(exps[layer, block : block + 1, lanes].astype(jnp.float32))
                part = codes[layer, block * BLOCK : (block + 1) * BLOCK, lanes]
                parts.append(part * scale.astype(part.dtype))
        blocks = jnp.concatenate(parts, axis=0).T.reshape(group, col_width, layers * rows)
        turned[pl.ds(chunk * group, group)] = blocks
    load_cmap.wait()
    load_order.wait()

    def gather(slot, o):
        to, to_g = peer(o)
        send[slot] = turned[cmap[to * g_size + to_g]]

    def copy(slot, o):
        return pltpu.make_async_remote_copy(
            src_ref=send.at[slot],
            dst_ref=recv.at[me],
            send_sem=send_sem,
            recv_sem=recv_sem,
            device_id=peer(o),
            device_id_type=MESH,
        )

    recv[me] = turned[cmap[me]]
    for slot, o in enumerate(column + rest):
        gather(slot, o)

    pl.semaphore_wait(barrier, len(greeted))
    line = [(0, 0, d, 0) for d in range(1, z_size)]
    for o in sorted(line, key=lambda o: -hops(o[2], z_size)):
        pl.semaphore_signal(line_sem, inc=1, device_id=peer(o), device_id_type=MESH)
    for slot, o in enumerate(column):
        copy(slot, o).start()
    pl.semaphore_wait(line_sem, len(line))
    for slot, o in enumerate(rest):
        here = (all_x[o[0]] == x).astype(jnp.int32) + (all_y[o[1]] == near_y[0]).astype(jnp.int32)
        pl.when(here < 2)(copy(len(column) + slot, o).start)

    others = recv.at[pl.ds(0, devices - 1)]
    pltpu.make_async_copy(others, others, recv_sem).wait()
    half = LANES // layers
    low = lax.broadcasted_iota(jnp.int32, (col_width, LANES), 1) < half

    @pl.loop(0, devices * half // LANES, unroll=32)
    def _(i):
        lanes = pl.ds(pl.multiple_of(i * LANES, LANES), LANES)
        a, b = recv[order[2 * i]], recv[order[2 * i + 1]]
        crossed = pltpu.roll(jnp.where(low, b, a), half, 1)
        tiles[0, :, lanes] = jnp.where(low, a, crossed)
        tiles[1, :, lanes] = jnp.where(low, crossed, b)

    pltpu.make_async_copy(others, others, send_sem).wait()


def assemble(tiles, rollout, sums, totals, out_sem):
    layers, col_width, width = rollout.shape
    quad = 2 * LANES
    span = LANES * BLOCK
    copies = []
    for i in range(width // span):
        lanes = pl.ds(i * span, span)
        copies.append(pltpu.make_async_copy(tiles.at[:, :, lanes], rollout.at[:, :, lanes], out_sem.at[i]))
        copies[-1].start()
    lane = lax.broadcasted_iota(jnp.int32, (col_width, LANES), 1)
    sources = lax.broadcasted_iota(jnp.int32, (quad, LANES), 0) // BLOCK
    targets = lax.broadcasted_iota(jnp.int32, (quad, LANES), 1) % (quad // BLOCK)
    picks = (sources == targets).astype(jnp.bfloat16)
    for start in range(0, width, span):
        for layer in range(layers):
            stacked = jnp.concatenate(
                [tiles[layer, :, at : at + quad] for at in range(start, start + span, quad)], axis=0
            )
            got = jnp.dot(stacked, picks, preferred_element_type=jnp.float32)
            got = got.reshape(span // quad, col_width, LANES)
            total = got[0]
            for i in range(1, span // quad):
                total = jnp.where(lane // (quad // BLOCK) == i, got[i], total)
            totals[layer, :, start // BLOCK : start // BLOCK + LANES] = total
    copies.append(pltpu.make_async_copy(totals, sums, out_sem.at[width // span]))
    copies[-1].start()
    for copy in copies:
        copy.wait()


def shards(sizes, codes, exponents, column_map, row_order):
    layers, rows, width = codes.shape
    devices = sizes[0] * sizes[1] * sizes[2] * sizes[3]
    column = sizes[2] * sizes[3]
    col_width = width // devices
    anywhere = pl.BlockSpec(memory_space=pl.ANY)
    tiled = (layers, col_width, devices * rows)
    tiles = pl.pallas_call(
        functools.partial(exchange, sizes),
        out_shape=pltpu.VMEM(tiled, jnp.bfloat16),
        in_specs=[anywhere] * 4,
        out_specs=pl.BlockSpec(memory_space=pltpu.VMEM),
        scratch_shapes=[
            pltpu.VMEM(codes.shape, codes.dtype),
            pltpu.VMEM(exponents.shape, exponents.dtype),
            pltpu.SMEM(column_map.shape, column_map.dtype),
            pltpu.SMEM(row_order.shape, row_order.dtype),
            pltpu.VMEM((devices, col_width, layers * rows), codes.dtype),
            pltpu.VMEM((devices + column - 1, col_width, layers * rows), jnp.bfloat16),
            pltpu.VMEM((devices, col_width, layers * rows), jnp.bfloat16),
            pltpu.SemaphoreType.DMA((5,)),
            pltpu.SemaphoreType.DMA(()),
            pltpu.SemaphoreType.DMA(()),
            pltpu.SemaphoreType.REGULAR,
        ],
        compiler_params=pltpu.CompilerParams(
            collective_id=0, has_side_effects=True, vmem_limit_bytes=60 << 20
        ),
        name="exchange",
    )(codes, exponents, column_map, row_order)
    rollout = jax.ShapeDtypeStruct(tiled, jnp.bfloat16)
    sums = jax.ShapeDtypeStruct((layers, col_width, devices * rows // BLOCK), jnp.float32)
    return pl.pallas_call(
        assemble,
        out_shape=(rollout, sums),
        in_specs=[
            pl.BlockSpec(memory_space=pltpu.VMEM),
        ],
        out_specs=(anywhere, anywhere),
        scratch_shapes=[
            pltpu.VMEM(sums.shape, sums.dtype),
            pltpu.SemaphoreType.DMA((5,)),
        ],
        compiler_params=pltpu.CompilerParams(vmem_limit_bytes=16 << 20),
        name="assemble",
    )(tiles)


def solution(mesh):
    chain, grp = mesh.shape["chain"], mesh.shape["grp"]
    z_size = next(n for n in range(1, chain + 1) if n ** 3 >= 4 * chain)
    side = 1
    while side * side * z_size < chain:
        side += 1
    sizes = (side, side, z_size, grp)
    assert side * side * z_size == chain
    return jax.shard_map(
        functools.partial(shards, sizes),
        mesh=mesh,
        in_specs=(P(None, ("chain", "grp"), None), P(None, ("chain", "grp"), None), P(), P()),
        out_specs=(P(None, ("chain", "grp"), None), P(None, ("chain", "grp"), None)),
        check_vma=False,
    )
```

```python
import functools

import jax
import jax.numpy as jnp
from jax import lax
from jax.experimental import pallas as pl
from jax.experimental.pallas import tpu as pltpu
from jax.sharding import PartitionSpec as P

MESH = pl.DeviceIdType.MESH
BLOCK = 32
LANES = 128


def hops(d, size):
    return min(d, size - d)


def plan(sizes):
    x_size, y_size, z_size, g_size = sizes
    offsets = [
        (dx, dy, dz, dg)
        for dg in range(g_size)
        for dy in range(y_size)
        for dx in range(x_size)
        for dz in range(z_size)
    ]

    def distance(o):
        return hops(o[0], x_size) + hops(o[1], y_size) + hops(o[2], z_size)

    side = [o for o in offsets if o[:2] in ((1, 0), (3, 0)) and o[2] in (3, 5)]
    greeted = [o for o in offsets[1:] if o[:2] == (0, 0) or o[2] == 0] + side
    greeted = sorted(greeted, key=lambda o: -distance(o))
    column = [o for o in offsets[1:] if o[:2] == (0, 0)]
    base = sorted(offsets, key=lambda o: ([0,2,1,3][o[1]],o[0],o[3],o[2]))
    place = {
        o + (0,): i / len(offsets)
        + 0.07 * (o[0] >= x_size // 2) + 0.2 * (o[1] >= y_size // 2) + 0.3 * (o[2] >= z_size // 2)
        for i, o in enumerate(base)
    }
    return greeted, column, side, sorted(place, key=lambda o: place[o])


def exchange(sizes, codes_hbm, exps_hbm, cmap_hbm, order_hbm, tiles, codes, exps, cmap, order, turned, send, recv, load_sem, send_sem, recv_sem, line_sem):
    x_size, y_size, z_size, g_size = sizes
    devices = x_size * y_size * z_size * g_size
    layers, rows, width = codes.shape
    col_width = width // devices
    greeted, column, side, rest = plan(sizes)
    first = column + side

    chain, g = lax.axis_index("chain"), lax.axis_index("grp")
    x, z = lax.rem(chain, x_size), lax.rem(lax.div(chain, x_size), z_size)
    y = lax.div(chain, x_size * z_size)
    me = chain * g_size + g
    cores = [lax.rem(g + d, g_size) for d in range(g_size)]

    def relative(at, size, step):
        return [lax.rem(at + d, size) * step for d in range(size)]

    def halved(at, size, step):
        half = size // 2
        turn = lax.rem(at, half)
        return [(h * half + lax.rem(turn + i, half)) * step for h in range(2) for i in range(half)]

    steps = ((x, x_size, 1), (y, y_size, x_size * z_size), (z, z_size, x_size))
    near_x, near_y, near_z = (relative(*s) for s in steps)
    all_x, all_y, all_z = (halved(*s) for s in steps)

    def peer(o):
        if len(o) == 4:
            return near_y[o[1]] + near_x[o[0]] + near_z[o[2]], cores[o[3]]
        return all_y[o[1]] + all_x[o[0]] + all_z[o[2]], cores[o[3]]

    barrier = pltpu.get_barrier_semaphore()
    for o in greeted:
        pl.semaphore_signal(barrier, inc=1, device_id=peer(o), device_id_type=MESH)

    pieces = 2
    piece = width // pieces
    load_exps = pltpu.make_async_copy(exps_hbm, exps, load_sem.at[pieces])
    load_exps.start()
    loads = []
    for i in range(pieces):
        lanes = pl.ds(i * piece, piece)
        loads.append(pltpu.make_async_copy(codes_hbm.at[:, :, lanes], codes.at[:, :, lanes], load_sem.at[i]))
        loads[-1].start()
    load_cmap = pltpu.make_async_copy(cmap_hbm, cmap, load_sem.at[pieces + 1])
    load_cmap.start()
    load_order = pltpu.make_async_copy(order_hbm, order, load_sem.at[pieces + 2])
    load_order.start()

    load_exps.wait()
    group = LANES // 8
    span = group * col_width
    for chunk in range(width // span):
        if chunk * span % piece == 0:
            loads[chunk * span // piece].wait()
        lanes = pl.ds(chunk * span, span)
        parts = []
        for layer in range(layers):
            for block in range(rows // BLOCK):
                scale = jnp.exp2(exps[layer, block : block + 1, lanes].astype(jnp.float32))
                part = codes[layer, block * BLOCK : (block + 1) * BLOCK, lanes]
                parts.append(part * scale.astype(part.dtype))
        blocks = jnp.concatenate(parts, axis=0).T.reshape(group, col_width, layers * rows)
        turned[pl.ds(chunk * group, group)] = blocks
    load_cmap.wait()
    load_order.wait()

    def gather(slot, o):
        to, to_g = peer(o)
        send[slot] = turned[cmap[to * g_size + to_g]]

    def copy(slot, o):
        return pltpu.make_async_remote_copy(
            src_ref=send.at[slot],
            dst_ref=recv.at[me],
            send_sem=send_sem,
            recv_sem=recv_sem,
            device_id=peer(o),
            device_id_type=MESH,
        )

    recv[me] = turned[cmap[me]]
    for slot, o in enumerate(first + rest):
        gather(slot, o)

    pl.semaphore_wait(barrier, len(greeted))
    line = [(0, 0, d, 0) for d in range(1, z_size)]
    for o in sorted(line, key=lambda o: -hops(o[2], z_size)):
        pl.semaphore_signal(line_sem, inc=1, device_id=peer(o), device_id_type=MESH)
    for slot, o in enumerate(first):
        copy(slot, o).start()
    pl.semaphore_wait(line_sem, len(line))
    same_x, same_y = ([(at == near[0]).astype(jnp.int32) for at in every] for every, near in ((all_x, near_x), (all_y, near_y)))
    side_columns = sorted({o[:2] for o in side})
    side_depths = sorted({o[2] for o in side})
    own, aside = {}, {}
    for jx in range(x_size):
        for jy in range(y_size):
            own[jx, jy] = same_x[jx] * same_y[jy]
            hits = [(all_x[jx] == near_x[dx]).astype(jnp.int32) * (all_y[jy] == near_y[dy]).astype(jnp.int32) for dx, dy in side_columns]
            aside[jx, jy] = sum(hits)
    deep = [sum((at == near_z[d]).astype(jnp.int32) for d in side_depths) for at in all_z]
    for slot, o in enumerate(rest):
        sent = own[o[0], o[1]] + aside[o[0], o[1]] * deep[o[2]]
        pl.when(sent == 0)(copy(len(first) + slot, o).start)

    others = recv.at[pl.ds(0, devices - 1)]
    pltpu.make_async_copy(others, others, recv_sem).wait()
    half = LANES // layers
    low = lax.broadcasted_iota(jnp.int32, (col_width, LANES), 1) < half

    @pl.loop(0, devices * half // LANES, unroll=32)
    def _(i):
        lanes = pl.ds(pl.multiple_of(i * LANES, LANES), LANES)
        a, b = recv[order[2 * i]], recv[order[2 * i + 1]]
        crossed = pltpu.roll(jnp.where(low, b, a), half, 1)
        tiles[0, :, lanes] = jnp.where(low, a, crossed)
        tiles[1, :, lanes] = jnp.where(low, crossed, b)

    pltpu.make_async_copy(others, others, send_sem).wait()


def assemble(tiles, rollout, sums, totals, out_sem):
    layers, col_width, width = rollout.shape
    quad = 2 * LANES
    span = LANES * BLOCK
    copies = []
    for i in range(width // span):
        lanes = pl.ds(i * span, span)
        copies.append(pltpu.make_async_copy(tiles.at[:, :, lanes], rollout.at[:, :, lanes], out_sem.at[i]))
        copies[-1].start()
    lane = lax.broadcasted_iota(jnp.int32, (col_width, LANES), 1)
    sources = lax.broadcasted_iota(jnp.int32, (quad, LANES), 0) // BLOCK
    targets = lax.broadcasted_iota(jnp.int32, (quad, LANES), 1) % (quad // BLOCK)
    picks = (sources == targets).astype(jnp.bfloat16)
    for start in range(0, width, span):
        for layer in range(layers):
            stacked = jnp.concatenate(
                [tiles[layer, :, at : at + quad] for at in range(start, start + span, quad)], axis=0
            )
            got = jnp.dot(stacked, picks, preferred_element_type=jnp.float32)
            got = got.reshape(span // quad, col_width, LANES)
            total = got[0]
            for i in range(1, span // quad):
                total = jnp.where(lane // (quad // BLOCK) == i, got[i], total)
            totals[layer, :, start // BLOCK : start // BLOCK + LANES] = total
    copies.append(pltpu.make_async_copy(totals, sums, out_sem.at[width // span]))
    copies[-1].start()
    for copy in copies:
        copy.wait()


def shards(sizes, codes, exponents, column_map, row_order):
    layers, rows, width = codes.shape
    devices = sizes[0] * sizes[1] * sizes[2] * sizes[3]
    greeted, column, side, rest = plan(sizes)
    first = len(column + side)
    col_width = width // devices
    anywhere = pl.BlockSpec(memory_space=pl.ANY)
    tiled = (layers, col_width, devices * rows)
    tiles = pl.pallas_call(
        functools.partial(exchange, sizes),
        out_shape=pltpu.VMEM(tiled, jnp.bfloat16),
        in_specs=[anywhere] * 4,
        out_specs=pl.BlockSpec(memory_space=pltpu.VMEM),
        scratch_shapes=[
            pltpu.VMEM(codes.shape, codes.dtype),
            pltpu.VMEM(exponents.shape, exponents.dtype),
            pltpu.SMEM(column_map.shape, column_map.dtype),
            pltpu.SMEM(row_order.shape, row_order.dtype),
            pltpu.VMEM((devices, col_width, layers * rows), codes.dtype),
            pltpu.VMEM((devices + first, col_width, layers * rows), jnp.bfloat16),
            pltpu.VMEM((devices, col_width, layers * rows), jnp.bfloat16),
            pltpu.SemaphoreType.DMA((5,)),
            pltpu.SemaphoreType.DMA(()),
            pltpu.SemaphoreType.DMA(()),
            pltpu.SemaphoreType.REGULAR,
        ],
        compiler_params=pltpu.CompilerParams(
            collective_id=0, has_side_effects=True, vmem_limit_bytes=60 << 20
        ),
        name="exchange",
    )(codes, exponents, column_map, row_order)
    rollout = jax.ShapeDtypeStruct(tiled, jnp.bfloat16)
    sums = jax.ShapeDtypeStruct((layers, col_width, devices * rows // BLOCK), jnp.float32)
    return pl.pallas_call(
        assemble,
        out_shape=(rollout, sums),
        in_specs=[
            pl.BlockSpec(memory_space=pltpu.VMEM),
        ],
        out_specs=(anywhere, anywhere),
        scratch_shapes=[
            pltpu.VMEM(sums.shape, sums.dtype),
            pltpu.SemaphoreType.DMA((5,)),
        ],
        compiler_params=pltpu.CompilerParams(vmem_limit_bytes=16 << 20),
        name="assemble",
    )(tiles)


def solution(mesh):
    chain, grp = mesh.shape["chain"], mesh.shape["grp"]
    z_size = next(n for n in range(1, chain + 1) if n ** 3 >= 4 * chain)
    side = 1
    while side * side * z_size < chain:
        side += 1
    sizes = (side, side, z_size, grp)
    assert side * side * z_size == chain
    return jax.shard_map(
        functools.partial(shards, sizes),
        mesh=mesh,
        in_specs=(P(None, ("chain", "grp"), None), P(None, ("chain", "grp"), None), P(), P()),
        out_specs=(P(None, ("chain", "grp"), None), P(None, ("chain", "grp"), None)),
        check_vma=False,
    )
```

```python
import functools

import jax
import jax.numpy as jnp
from jax import lax
from jax.experimental import pallas as pl
from jax.experimental.pallas import tpu as pltpu
from jax.sharding import PartitionSpec as P

MESH = pl.DeviceIdType.MESH
BLOCK = 32
LANES = 128


def hops(d, size):
    return min(d, size - d)


def plan(sizes):
    x_size, y_size, z_size, g_size = sizes
    offsets = [
        (dx, dy, dz, dg)
        for dg in range(g_size)
        for dy in range(y_size)
        for dx in range(x_size)
        for dz in range(z_size)
    ]

    def distance(o):
        return hops(o[0], x_size) + hops(o[1], y_size) + hops(o[2], z_size)

    side = [o for o in offsets if o[:2] in ((1, 0), (3, 0)) and o[2] in (3, 5)]
    greeted = [o for o in offsets[1:] if o[:2] == (0, 0) or o[2] == 0] + side
    greeted = sorted(greeted, key=lambda o: -distance(o))
    column = [o for o in offsets[1:] if o[:2] == (0, 0)]
    base = sorted(offsets, key=lambda o: ([0,2,1,3][o[1]],o[0],o[3],o[2]))
    place = {
        o + (0,): i / len(offsets)
        + 0.07 * (o[0] >= x_size // 2) + 0.2 * (o[1] >= y_size // 2) + 0.3 * (o[2] >= z_size // 2)
        for i, o in enumerate(base)
    }
    return greeted, column, side, sorted(place, key=lambda o: place[o])


def exchange(sizes, codes_hbm, exps_hbm, cmap_hbm, order_hbm, tiles, codes, exps, cmap, order, turned, send, recv, load_sem, send_sem, recv_sem, line_sem):
    x_size, y_size, z_size, g_size = sizes
    devices = x_size * y_size * z_size * g_size
    layers, rows, width = codes.shape
    col_width = width // devices
    greeted, column, side, rest = plan(sizes)
    first = column + side

    chain, g = lax.axis_index("chain"), lax.axis_index("grp")
    x, z = lax.rem(chain, x_size), lax.rem(lax.div(chain, x_size), z_size)
    y = lax.div(chain, x_size * z_size)
    me = chain * g_size + g
    cores = [lax.rem(g + d, g_size) for d in range(g_size)]

    def relative(at, size, step):
        return [lax.rem(at + d, size) * step for d in range(size)]

    def halved(at, size, step):
        half = size // 2
        turn = lax.rem(at, half)
        return [(h * half + lax.rem(turn + i, half)) * step for h in range(2) for i in range(half)]

    steps = ((x, x_size, 1), (y, y_size, x_size * z_size), (z, z_size, x_size))
    near_x, near_y, near_z = (relative(*s) for s in steps)
    all_x, all_y, all_z = (halved(*s) for s in steps)

    def peer(o):
        if len(o) == 4:
            return near_y[o[1]] + near_x[o[0]] + near_z[o[2]], cores[o[3]]
        return all_y[o[1]] + all_x[o[0]] + all_z[o[2]], cores[o[3]]

    barrier = pltpu.get_barrier_semaphore()
    for o in greeted:
        pl.semaphore_signal(barrier, inc=1, device_id=peer(o), device_id_type=MESH)

    pieces = 2
    piece = width // pieces
    load_exps = pltpu.make_async_copy(exps_hbm, exps, load_sem.at[pieces])
    load_exps.start()
    loads = []
    for i in range(pieces):
        lanes = pl.ds(i * piece, piece)
        loads.append(pltpu.make_async_copy(codes_hbm.at[:, :, lanes], codes.at[:, :, lanes], load_sem.at[i]))
        loads[-1].start()
    load_cmap = pltpu.make_async_copy(cmap_hbm, cmap, load_sem.at[pieces + 1])
    load_cmap.start()
    load_order = pltpu.make_async_copy(order_hbm, order, load_sem.at[pieces + 2])
    load_order.start()

    load_exps.wait()
    group = LANES // 8
    span = group * col_width
    for chunk in range(width // span):
        if chunk * span % piece == 0:
            loads[chunk * span // piece].wait()
        lanes = pl.ds(chunk * span, span)
        parts = []
        for layer in range(layers):
            for block in range(rows // BLOCK):
                scale = jnp.exp2(exps[layer, block : block + 1, lanes].astype(jnp.float32))
                part = codes[layer, block * BLOCK : (block + 1) * BLOCK, lanes]
                parts.append(part * scale.astype(part.dtype))
        blocks = jnp.concatenate(parts, axis=0).T.reshape(group, col_width, layers * rows)
        turned[pl.ds(chunk * group, group)] = blocks
    load_cmap.wait()
    load_order.wait()

    def gather(slot, o):
        to, to_g = peer(o)
        send[slot] = turned[cmap[to * g_size + to_g]]

    def copy(slot, o):
        return pltpu.make_async_remote_copy(
            src_ref=send.at[slot],
            dst_ref=recv.at[me],
            send_sem=send_sem,
            recv_sem=recv_sem,
            device_id=peer(o),
            device_id_type=MESH,
        )

    recv[me] = turned[cmap[me]]
    for slot, o in enumerate(first + rest):
        gather(slot, o)

    pl.semaphore_wait(barrier, len(greeted))
    line = [(0, 0, d, 0) for d in range(1, z_size)]
    for o in sorted(line, key=lambda o: -hops(o[2], z_size)):
        pl.semaphore_signal(line_sem, inc=1, device_id=peer(o), device_id_type=MESH)
    for slot, o in enumerate(first):
        copy(slot, o).start()
    pl.semaphore_wait(line_sem, len(line))
    same_x, same_y = ([(at == near[0]).astype(jnp.int32) for at in every] for every, near in ((all_x, near_x), (all_y, near_y)))
    side_columns = sorted({o[:2] for o in side})
    side_depths = sorted({o[2] for o in side})
    own, aside = {}, {}
    for jx in range(x_size):
        for jy in range(y_size):
            own[jx, jy] = same_x[jx] * same_y[jy]
            hits = [(all_x[jx] == near_x[dx]).astype(jnp.int32) * (all_y[jy] == near_y[dy]).astype(jnp.int32) for dx, dy in side_columns]
            aside[jx, jy] = sum(hits)
    deep = [sum((at == near_z[d]).astype(jnp.int32) for d in side_depths) for at in all_z]
    for slot, o in enumerate(rest):
        sent = own[o[0], o[1]] + aside[o[0], o[1]] * deep[o[2]]
        pl.when(sent == 0)(copy(len(first) + slot, o).start)

    others = recv.at[pl.ds(0, devices - 1)]
    pltpu.make_async_copy(others, others, recv_sem).wait()
    half = LANES // layers
    low = lax.broadcasted_iota(jnp.int32, (col_width, LANES), 1) < half

    @pl.loop(0, devices * half // (4 * LANES), unroll=8)
    def _(i):
        lanes = pl.ds(pl.multiple_of(i * 4 * LANES, 4 * LANES), 4 * LANES)
        lows, highs = [], []
        for j in range(4):
            a, b = recv[order[8 * i + 2 * j]], recv[order[8 * i + 2 * j + 1]]
            crossed = pltpu.roll(jnp.where(low, b, a), half, 1)
            lows.append(jnp.where(low, a, crossed))
            highs.append(jnp.where(low, crossed, b))
        tiles[0, :, lanes] = jnp.concatenate(lows, axis=1)
        tiles[1, :, lanes] = jnp.concatenate(highs, axis=1)

    pltpu.make_async_copy(others, others, send_sem).wait()


def assemble(tiles, rollout, sums, totals, out_sem):
    layers, col_width, width = rollout.shape
    quad = 2 * LANES
    span = LANES * BLOCK
    copies = []
    for i in range(width // span):
        lanes = pl.ds(i * span, span)
        copies.append(pltpu.make_async_copy(tiles.at[:, :, lanes], rollout.at[:, :, lanes], out_sem.at[i]))
        copies[-1].start()
    lane = lax.broadcasted_iota(jnp.int32, (col_width, LANES), 1)
    sources = lax.broadcasted_iota(jnp.int32, (quad, LANES), 0) // BLOCK
    targets = lax.broadcasted_iota(jnp.int32, (quad, LANES), 1) % (quad // BLOCK)
    picks = (sources == targets).astype(jnp.bfloat16)
    for start in range(0, width, span):
        for layer in range(layers):
            stacked = jnp.concatenate(
                [tiles[layer, :, at : at + quad] for at in range(start, start + span, quad)], axis=0
            )
            got = jnp.dot(stacked, picks, preferred_element_type=jnp.float32)
            got = got.reshape(span // quad, col_width, LANES)
            total = got[0]
            for i in range(1, span // quad):
                total = jnp.where(lane // (quad // BLOCK) == i, got[i], total)
            totals[layer, :, start // BLOCK : start // BLOCK + LANES] = total
    copies.append(pltpu.make_async_copy(totals, sums, out_sem.at[width // span]))
    copies[-1].start()
    for copy in copies:
        copy.wait()


def shards(sizes, codes, exponents, column_map, row_order):
    layers, rows, width = codes.shape
    devices = sizes[0] * sizes[1] * sizes[2] * sizes[3]
    greeted, column, side, rest = plan(sizes)
    first = len(column + side)
    col_width = width // devices
    anywhere = pl.BlockSpec(memory_space=pl.ANY)
    tiled = (layers, col_width, devices * rows)
    tiles = pl.pallas_call(
        functools.partial(exchange, sizes),
        out_shape=pltpu.VMEM(tiled, jnp.bfloat16),
        in_specs=[anywhere] * 4,
        out_specs=pl.BlockSpec(memory_space=pltpu.VMEM),
        scratch_shapes=[
            pltpu.VMEM(codes.shape, codes.dtype),
            pltpu.VMEM(exponents.shape, exponents.dtype),
            pltpu.SMEM(column_map.shape, column_map.dtype),
            pltpu.SMEM(row_order.shape, row_order.dtype),
            pltpu.VMEM((devices, col_width, layers * rows), codes.dtype),
            pltpu.VMEM((devices + first, col_width, layers * rows), jnp.bfloat16),
            pltpu.VMEM((devices, col_width, layers * rows), jnp.bfloat16),
            pltpu.SemaphoreType.DMA((5,)),
            pltpu.SemaphoreType.DMA(()),
            pltpu.SemaphoreType.DMA(()),
            pltpu.SemaphoreType.REGULAR,
        ],
        compiler_params=pltpu.CompilerParams(
            collective_id=0, has_side_effects=True, vmem_limit_bytes=60 << 20
        ),
        name="exchange",
    )(codes, exponents, column_map, row_order)
    rollout = jax.ShapeDtypeStruct(tiled, jnp.bfloat16)
    sums = jax.ShapeDtypeStruct((layers, col_width, devices * rows // BLOCK), jnp.float32)
    return pl.pallas_call(
        assemble,
        out_shape=(rollout, sums),
        in_specs=[
            pl.BlockSpec(memory_space=pltpu.VMEM),
        ],
        out_specs=(anywhere, anywhere),
        scratch_shapes=[
            pltpu.VMEM(sums.shape, sums.dtype),
            pltpu.SemaphoreType.DMA((5,)),
        ],
        compiler_params=pltpu.CompilerParams(vmem_limit_bytes=16 << 20),
        name="assemble",
    )(tiles)


def solution(mesh):
    chain, grp = mesh.shape["chain"], mesh.shape["grp"]
    z_size = next(n for n in range(1, chain + 1) if n ** 3 >= 4 * chain)
    side = 1
    while side * side * z_size < chain:
        side += 1
    sizes = (side, side, z_size, grp)
    assert side * side * z_size == chain
    return jax.shard_map(
        functools.partial(shards, sizes),
        mesh=mesh,
        in_specs=(P(None, ("chain", "grp"), None), P(None, ("chain", "grp"), None), P(), P()),
        out_specs=(P(None, ("chain", "grp"), None), P(None, ("chain", "grp"), None)),
        check_vma=False,
    )
```
